32 devices in a mesh: lat: 8 (over z, y), lon: 4 (over x, core).
Axes of the slice: x: 2, y: 2, z: 4, core: 2. Of those that a mesh axis runs over, the one named last changes fastest.
Arguments:
- features: bfloat16 [98304, 128], P(('lat', 'lon')), may hold values from -6 to 6
- cell_index: int32 [98304], P(('lat', 'lon')), may hold values from 0 to 2547
- tile_rows: int32 [1024], P(('lat', 'lon')), may hold values from 1 to 96, as said below
- spread: float32 [3, 3], replicated, may hold values from 0.2 to 1
- w_in: bfloat16 [128, 256], replicated, may hold values from -0.5 to 0.5
- w_dens: float32 [256], replicated, may hold values from -3 to 3
- w_one: bfloat16 [3, 3, 256, 256], replicated, may hold values from -0.125 to 0.125
- w_two: bfloat16 [3, 3, 256, 256], replicated, may hold values from -0.125 to 0.125
Outputs:
- encoded: bfloat16 [192, 384, 256], P('lat', 'lon')
The draws below stay inside these ranges and needn't reach their ends.
Inputs may be any that keep to these rules, and one draw needn't show every extreme that they name: `tile_rows`: every block has 1 to 96 used slots; on every device some block has exactly 96.
All inputs are finite; a program needn't handle non-finite values.
Results may differ from the reference program's by a relative error of at most 0.0054.
Values may be sent and summed in bfloat16 or wider, within the bound.
A program may use at most 64 MiB of HBM per device.

```python
import math
import jax
import jax.numpy as jnp
from jax import lax

TH = 24
TW = 96
F = 128
C = 256
CAP = 96
TILES = 32
OBS_ALL = 98304
PH = 26
PW = 98
GH = 192
GW = 384
N_LAT = 8
N_LON = 4
DEVICES = 32


def draw_tile_rows(key, part):
    heat = jax.random.randint(jax.random.fold_in(key, 11), (TILES,), 1, 5)
    low = jnp.maximum(1, heat * CAP // 8)
    high = heat * CAP // 4 + 1
    counts = jax.random.randint(jax.random.fold_in(key, 12), (DEVICES, TILES), low[None, :], high[None, :])
    counts = jnp.minimum(counts, CAP)
    forced = jax.random.randint(jax.random.fold_in(key, 13), (DEVICES,), 0, TILES)
    tile_ids = jnp.arange(TILES, dtype=jnp.int32)
    counts = jnp.where(tile_ids[None, :] == forced[:, None], CAP, counts)
    return counts.reshape(DEVICES * TILES).astype(jnp.int32)


def with_ends(entries, own_key, smallest, largest):
    longest = entries.shape.index(max(entries.shape))
    spots = []
    for shift in (0, 1):
        where = [jax.random.randint(jax.random.fold_in(own_key, axis), (), 0, length) for axis, length in enumerate(entries.shape)]
        where[longest] = (where[longest] + shift) % entries.shape[longest]
        spots.append(tuple(where))
    return entries.at[spots[0]].set(smallest).at[spots[1]].set(largest)


def level_of(key, extent, cuts, low, high):
    gain, own = 1.0, jax.random.fold_in(key, 6)
    for position, blocks in cuts:
        steps = jnp.exp(jax.random.uniform(jax.random.fold_in(own, position), (blocks,), jnp.float32, low / len(cuts), high / len(cuts)))
        gain = gain * jnp.repeat(steps, extent[position] // blocks).reshape([-1 if axis == position else 1 for axis in range(len(extent))])
    return gain


def bell_draw(key, shape, scale, limit, cuts=(), held_as=jnp.bfloat16):
    values = jax.random.normal(key, shape, jnp.float32) * scale
    if len(cuts) > 0:
        values = level_of(key, shape, cuts, -0.22, 0.18) * values
    return jnp.clip(values, min=-limit, max=limit).astype(held_as)


def setup_inputs(seed: int = 0) -> dict:
    seeds = jax.random.split(jax.random.key(seed), 9)
    return {
        "features": bell_draw(seeds[0], (OBS_ALL, F), 1.0, 6.0, ((0, 32),)),
        "cell_index": with_ends(jax.random.randint(seeds[1], (OBS_ALL,), 0, PH * PW), jax.random.fold_in(seeds[1], 1), 0, (PH * PW) - 1).astype(jnp.int32),
        "tile_rows": draw_tile_rows(jax.random.fold_in(seeds[8], 71), 0),
        "spread": jnp.clip(jnp.exp(jax.random.uniform(seeds[3], (3, 3), jnp.float32, math.log(0.2), math.log(1.0))), 0.2, 1.0),
        "w_in": bell_draw(seeds[4], (F, C), F ** -0.5, 0.5),
        "w_dens": bell_draw(seeds[5], (C,), 0.5, 3.0, (), jnp.float32),
        "w_one": bell_draw(seeds[6], (3, 3, C, C), (9 * C) ** -0.5, 0.125),
        "w_two": bell_draw(seeds[7], (3, 3, C, C), (9 * C) ** -0.5, 0.125),
    }


def wrap_pad(field):
    cols = jnp.concatenate([field[:, -1:], field, field[:, :1]], axis=1)
    return jnp.pad(cols, ((1, 1), (0, 0), (0, 0)))


def conv_grid(field, weight):
    padded = wrap_pad(field)
    rows_all, cols_all, chans = field.shape
    total = jnp.zeros((rows_all * cols_all, weight.shape[3]), jnp.float32)
    for row_off in range(3):
        for col_off in range(3):
            window = padded[row_off:row_off + rows_all, col_off:col_off + cols_all].reshape(-1, chans)
            total = total + jnp.dot(window, weight[row_off, col_off], preferred_element_type=jnp.float32)
    return total.reshape(rows_all, cols_all, -1)


def reference(features, cell_index, tile_rows, spread, w_in, w_dens, w_one, w_two):
    tiles = N_LAT * N_LON
    frame_cells = PH * PW
    blocks = features.reshape(DEVICES, tiles, CAP, F)
    cell_blocks = cell_index.reshape(DEVICES, tiles, CAP)
    counts = tile_rows.reshape(DEVICES, tiles)
    slot_ids = jnp.arange(CAP, dtype=jnp.int32)

    def one_tile(tile):
        rows = lax.dynamic_index_in_dim(blocks, tile, 1, keepdims=False)
        cells = lax.dynamic_index_in_dim(cell_blocks, tile, 1, keepdims=False)
        used = lax.dynamic_index_in_dim(counts, tile, 1, keepdims=False)
        valid = slot_ids[None, :] < used[:, None]
        segment = jnp.where(valid, cells, frame_cells).reshape(-1).astype(jnp.int32)
        sums = jax.ops.segment_sum(rows.reshape(-1, F).astype(jnp.float32), segment, num_segments=frame_cells + 1)
        numbers = jax.ops.segment_sum(jnp.ones(segment.shape, jnp.float32), segment, num_segments=frame_cells + 1)
        return sums[:frame_cells], numbers[:frame_cells]

    frame_sum, frame_count = lax.map(one_tile, jnp.arange(tiles, dtype=jnp.int32))
    frame_sum = frame_sum.reshape(tiles, PH, PW, F)
    frame_count = frame_count.reshape(tiles, PH, PW)
    data = jnp.zeros((tiles, TH, TW, F), jnp.float32)
    density = jnp.zeros((tiles, TH, TW), jnp.float32)
    for row_off in range(3):
        for col_off in range(3):
            data = data + spread[row_off, col_off] * frame_sum[:, row_off:row_off + TH, col_off:col_off + TW]
            density = density + spread[row_off, col_off] * frame_count[:, row_off:row_off + TH, col_off:col_off + TW]
    mean = (data / (1.0 + density)[..., None]).astype(jnp.bfloat16)
    grid = jnp.dot(mean.reshape(-1, F), w_in, preferred_element_type=jnp.float32)
    grid = grid + jnp.log1p(density).reshape(-1, 1) * w_dens[None, :]
    grid = grid.astype(jnp.bfloat16).reshape(N_LAT, N_LON, TH, TW, C)
    grid = jnp.transpose(grid, (0, 2, 1, 3, 4)).reshape(GH, GW, C)
    hidden = jax.nn.silu(conv_grid(grid, w_one)).astype(jnp.bfloat16)
    encoded = grid.astype(jnp.float32) + conv_grid(hidden, w_two)
    return encoded.astype(jnp.bfloat16)
```

```python
import functools

import jax
import jax.numpy as jnp
from jax import lax
from jax.experimental import pallas as pl
from jax.experimental.pallas import tpu as pltpu
from jax.sharding import PartitionSpec as P

TH = 24
TW = 96
F = 128
C = 256
CAP = 96
PH = 26
PW = 98
GROUP = 8
WIDE = GROUP * CAP
PASS = 256
BLOCKS = WIDE // 128
SLOTS = 3
SIDE = 32
COLS = (0, 1, TW - 2, TW - 1)
MESH = pl.DeviceIdType.MESH
F32 = jnp.float32
BF16 = jnp.bfloat16


def kernel(
    lat_n, lon_n,
    feats, raw, used, spread, w_in, w_dens, w_one, w_two, out,
    cells, cells_in, rows_in, taps, hots, lhs0, lhs1, lhs2, lhs_col, acc, acc_col, acc_row, count, log_in, log_out,
    rhs_v, inv_b, log_b, grid_x, hid_x, mean_out, mean_in, col_out, col_in, corner_out, corner_in, sides, hid_side,
    out_v, win_v, wone_v, wtwo_v,
    row_send, row_recv, cell_send, cell_recv, own_sem, w_sem, out_sem, halo_send, halo_recv,
):
    lhs = (lhs0, lhs1, lhs2)
    n = lat_n * lon_n
    groups = n // GROUP
    lat = lax.axis_index("lat")
    lon = lax.axis_index("lon")
    me = lat * lon_n + lon
    east = (lon + 1) % lon_n
    west = (lon + lon_n - 1) % lon_n

    log_in[...] = jnp.zeros_like(log_in)
    bits = [1 << k for k in range(n.bit_length() - 1)]
    flips = [bit * (1 - 2 * (me // bit % 2)) for bit in bits]

    def across(d):
        return me + sum((d // bit % 2) * flip for bit, flip in zip(bits, flips))

    barrier = pltpu.get_barrier_semaphore()

    @pl.loop(1, n)
    def _(k):
        peer = (me + k) % n
        pl.semaphore_signal(
            barrier, inc=1, device_id=(peer // lon_n, peer % lon_n), device_id_type=MESH
        )

    weights = [
        pltpu.make_async_copy(w_in, win_v, w_sem.at[0]),
        pltpu.make_async_copy(w_one, wone_v, w_sem.at[1]),
        pltpu.make_async_copy(w_two, wtwo_v, w_sem.at[2]),
    ]
    for item in weights:
        item.start()

    lane = lax.broadcasted_iota(jnp.int32, (1, 128), 1)

    @pl.loop(0, n // 4)
    def _(quad):
        one, two, three = (raw[pl.ds(3 * quad + k, 1)] for k in range(3))
        picks = [
            one,
            jnp.where(lane < 32, pltpu.roll(one, 32, 1), pltpu.roll(two, 32, 1)),
            jnp.where(lane < 64, pltpu.roll(two, 64, 1), pltpu.roll(three, 64, 1)),
            pltpu.roll(three, 96, 1),
        ]
        for k, pick in enumerate(picks):
            row = ((pick.astype(F32) + 0.5) * (1.0 / PW)).astype(jnp.int32)
            code = row * 128 + (pick - row * PW)
            cells[4 * quad + k] = jnp.where(lane < used[4 * quad + k], code, 127 * 128)

    own = [
        pltpu.make_async_copy(feats.at[me], rows_in.at[0], own_sem.at[0]),
        pltpu.make_async_copy(cells.at[me], cells_in.at[0], own_sem.at[1]),
    ]
    count[...] = jnp.zeros_like(count)
    pl.semaphore_wait(barrier, n - 1)

    def cell_copy(d, peer):
        return pltpu.make_async_remote_copy(
            src_ref=cells.at[peer], dst_ref=cells_in.at[d],
            send_sem=cell_send.at[d], recv_sem=cell_recv.at[d],
            device_id=(peer // lon_n, peer % lon_n), device_id_type=MESH,
        )

    def row_copy(d, peer):
        return pltpu.make_async_remote_copy(
            src_ref=feats.at[peer], dst_ref=rows_in.at[d],
            send_sem=row_send.at[d], recv_sem=row_recv.at[d],
            device_id=(peer // lon_n, peer % lon_n), device_id_type=MESH,
        )

    for d in range(1, n):
        cell_copy(d, across(d)).start()
    for d in range(1, n):
        row_copy(d, across(d)).start()

    for item in own:
        item.start()

    def codes(group):
        enc = jnp.concatenate([cells_in[group * GROUP + m][:, :CAP] for m in range(GROUP)], axis=1)
        return enc & 127, enc >> 7

    def prepare(group, slot):
        col, row = codes(group)
        reach = jnp.broadcast_to(col, (TW, WIDE)) - lax.broadcasted_iota(jnp.int32, (TW, WIDE), 0)
        for a in range(3):
            tap = jnp.where(reach == 2, spread[a, 2], 0.0)
            tap = jnp.where(reach == 1, spread[a, 1], tap)
            taps[a] = jnp.where(reach == 0, spread[a, 0], tap).astype(BF16)
        wide_row = jnp.broadcast_to(row, (16, WIDE))
        for r in range(PH):
            hots[r] = jnp.where(wide_row == r, 1.0, 0.0).astype(BF16)
        above = jnp.broadcast_to(row, (SIDE, WIDE)) - lax.broadcasted_iota(jnp.int32, (SIDE, WIDE), 0)
        for k, c in enumerate(COLS):
            total = jnp.zeros((SIDE, WIDE), F32)
            for a in range(3):
                line = jnp.where(col == c + 2, spread[a, 2], 0.0)
                line = jnp.where(col == c + 1, spread[a, 1], line)
                line = jnp.where(col == c, spread[a, 0], line)
                total = jnp.where(above == a - 2, jnp.broadcast_to(line, (SIDE, WIDE)), total)
            lhs_col[slot, SIDE * k : SIDE * (k + 1)] = total.astype(BF16)

    def fill(block, slot):
        lanes = pl.ds(pl.multiple_of(block * 128, 128), 128)
        hot = [hots[r, :, lanes] for r in range(PH)]
        for strip in range(TW // 16):
            lines = slice(strip * 16, strip * 16 + 16)
            zero, one, two = (taps[a, lines, lanes] for a in range(3))
            for i in range(TH):
                lhs[slot][i, lines, lanes] = zero * hot[i] + one * hot[i + 1] + two * hot[i + 2]

    def build(group, slot):
        prepare(group, slot)

        @pl.loop(0, BLOCKS)
        def _(block):
            fill(block, slot)

    def cells_arrive(lo, hi):
        @pl.loop(lo, hi)
        def _(d):
            cell_copy(d, across(d)).wait_recv()

    own[1].wait()
    cells_arrive(1, GROUP)
    build(0, 0)
    if groups > 1:
        cells_arrive(GROUP, 2 * GROUP)
        build(1, 1)
    if groups > 2:
        cells_arrive(2 * GROUP, n)

    @pl.loop(0, groups)
    def _(group):
        col, row = codes(group)
        row_hot = jnp.where(
            lax.broadcasted_iota(jnp.int32, (SIDE, WIDE), 0) == row, 1.0, 0.0
        ).astype(BF16)
        col_hot = jnp.where(
            lax.broadcasted_iota(jnp.int32, (128, WIDE), 0) == col, 1.0, 0.0
        ).astype(BF16)
        count[...] += lax.dot_general(
            row_hot, col_hot, (((1,), (1,)), ((), ())), preferred_element_type=F32
        )

    density = jnp.zeros((SIDE, 128), F32)
    for a in range(3):
        line = count[...] if a == 2 else pltpu.roll(count[...], 2 - a, 0)
        for b in range(3):
            density += spread[a, b] * (line if b == 0 else pltpu.roll(line, 128 - b, 1))
    level = 1.0 + density
    inverse = 1.0 / level
    logs = jnp.log(level)
    log_out[0] = logs[0:8]
    log_out[1] = logs[SIDE - 8 : SIDE]

    def halo_copy(kind, src, dst, where):
        return pltpu.make_async_remote_copy(
            src_ref=src, dst_ref=dst, send_sem=halo_send.at[kind], recv_sem=halo_recv.at[kind],
            device_id=where, device_id_type=MESH,
        )

    up, down = lat - 1, lat + 1
    log_up = [halo_copy(0, log_out.at[0], log_in.at[1], (up, lon))]
    log_down = [halo_copy(1, log_out.at[1], log_in.at[0], (down, lon))]
    to_up = [
        halo_copy(2, mean_out.at[0], mean_in.at[1], (up, lon)),
        halo_copy(6, corner_out.at[0], corner_in.at[2], (up, east)),
        halo_copy(7, corner_out.at[1], corner_in.at[3], (up, west)),
    ]
    to_down = [
        halo_copy(3, mean_out.at[1], mean_in.at[0], (down, lon)),
        halo_copy(8, corner_out.at[2], corner_in.at[0], (down, east)),
        halo_copy(9, corner_out.at[3], corner_in.at[1], (down, west)),
    ]
    beside = [
        halo_copy(4, col_out.at[pl.ds(2, 2)], col_in.at[0], (lat, east)),
        halo_copy(5, col_out.at[pl.ds(0, 2)], col_in.at[1], (lat, west)),
    ]

    def when_up(act):
        @pl.when(lat > 0)
        def _():
            act()

    def when_down(act):
        @pl.when(lat < lat_n - 1)
        def _():
            act()

    def start_all(items):
        def act():
            for item in items:
                item.start()
        return act

    when_up(start_all(log_up))
    when_down(start_all(log_down))

    def features_of(group, lo, size):
        low, high = lo // CAP, -(-(lo + size) // CAP)
        rows = rows_in[pl.ds(group * GROUP + low, high - low)].reshape((high - low) * CAP, F)
        return rows[lo - low * CAP : lo - low * CAP + size]

    def add(group, slot, lo, size, first):
        rows = features_of(group, lo, size)
        span = slice(lo, lo + size)
        rhs = jnp.dot(rows, win_v[...], preferred_element_type=F32).astype(BF16)
        step = 12
        for i in range(0, TH, step):
            part = jnp.dot(
                lhs[slot][i : i + step, :, span].reshape(step * TW, size), rhs,
                preferred_element_type=F32,
            ).reshape(step, TW, C)
            acc[i : i + step] = part if first else acc[i : i + step] + part
        add_border(slot, rows, rhs, span, first)

    def add_beside(group, slot, later, spare, first):
        rows = features_of(group, 0, WIDE)
        rhs_v[...] = jnp.dot(rows, win_v[...], preferred_element_type=F32).astype(BF16)
        prepare(later, spare)
        size = TH // BLOCKS

        @pl.loop(0, BLOCKS)
        def _(block):
            lines = pl.ds(block * size, size)
            part = jnp.dot(
                lhs[slot][lines].reshape(size * TW, WIDE), rhs_v[...], preferred_element_type=F32
            ).reshape(size, TW, C)
            acc[lines] = part if first else acc[lines] + part
            fill(block, spare)

        add_border(slot, rows, rhs_v[...], slice(0, WIDE), first)

    def add_border(slot, rows, rhs, span, first):
        part = jnp.dot(lhs_col[slot, :, span], rhs, preferred_element_type=F32)
        acc_col[...] = part if first else acc_col[...] + part
        size = rows.shape[0]
        for k, i in ((0, 0), (2, TH - 2)):
            part = jnp.dot(
                lhs[slot][i : i + 2, :, span].reshape(2 * TW, size), rows,
                preferred_element_type=F32,
            ).reshape(2, TW, F)
            acc_row[k : k + 2] = part if first else acc_row[k : k + 2] + part

    def arrive(d):
        row_copy(d, across(d)).wait_recv()

    weights[0].wait()

    def wait_all(items):
        def act():
            for item in items:
                item.wait_recv()
        return act

    own[0].wait()
    if groups > 2:
        for d in range(1, GROUP):
            arrive(d)
        add_beside(0, 0, 2, 2, True)

    turned = jnp.transpose(jnp.concatenate([logs, jnp.zeros((128 - SIDE, 128), F32)], axis=0))
    for i in range(TH):
        log_b[i] = jnp.broadcast_to(turned[:TW, i + 2 : i + 3], (TW, 128))
    turned = jnp.transpose(
        jnp.concatenate([inverse, jnp.zeros((128 - SIDE, 128), F32)], axis=0)
    )
    for i in range(TH):
        inv_b[i] = jnp.broadcast_to(turned[:TW, i + 2 : i + 3], (TW, 128))

    for group in range(1, groups - 2):
        for m in range(GROUP):
            arrive(group * GROUP + m)
        add_beside(group, group % SLOTS, group + 2, (group + 2) % SLOTS, False)

    last = groups - 1
    slot = last % SLOTS
    for group in range(max(groups - 2, 0), groups):
        ready = 1 if group == 0 else 0
        for lo in range(0, WIDE - (PASS if group == last else 0), PASS):
            need = -(-(lo + PASS) // CAP)
            for m in range(ready, need):
                arrive(group * GROUP + m)
            ready = need
            add(group, group % SLOTS, lo, PASS, group == 0 and lo == 0)
    for m in range(ready, GROUP):
        arrive(last * GROUP + m)
    tail = slice(WIDE - PASS, WIDE)
    rows = features_of(last, WIDE - PASS, PASS)
    rhs = jnp.dot(rows, win_v[...], preferred_element_type=F32).astype(BF16)

    def scaled(total, t):
        factor, lg = inv_b[t - 2], log_b[t - 2]
        return total * jnp.concatenate([factor, factor], axis=1) + jnp.concatenate(
            [lg, lg], axis=1
        ) * w_dens[...]

    for k, i in ((0, 0), (2, TH - 2)):
        part = jnp.dot(
            lhs[slot][i : i + 2, :, tail].reshape(2 * TW, PASS), rows, preferred_element_type=F32
        ).reshape(2, TW, F)
        for m in range(2):
            mean_out[k // 2, m] = ((acc_row[k + m] + part[m]) * inv_b[i + m]).astype(BF16)
    when_up(to_up[0].start)
    when_down(to_down[0].start)
    part = acc_col[...] + jnp.dot(lhs_col[slot, :, tail], rhs, preferred_element_type=F32)
    inside = lax.broadcasted_iota(jnp.int32, (SIDE, C), 0)
    inside = (inside >= 2) & (inside < TH + 2)
    border = []
    for k, c in enumerate(COLS):
        factor = jnp.broadcast_to(inverse[:, c : c + 1], (SIDE, C))
        lg = jnp.broadcast_to(logs[:, c : c + 1], (SIDE, C))
        value = part[SIDE * k : SIDE * (k + 1)] * factor + lg * w_dens[...]
        value = jnp.where(inside, value, 0.0)
        border.append(value)
        col_out[k] = value.astype(BF16)
        sides[2 + k] = value
    for item in beside:
        item.start()
    pad = jnp.zeros((4, C), F32)
    for k, (line, pair) in enumerate(((2, 2), (2, 0), (TH, 2), (TH, 0))):
        corner_out[k] = jnp.concatenate(
            [border[pair][line : line + 2], border[pair + 1][line : line + 2], pad], axis=0
        )
    when_up(start_all(to_up[1:]))
    when_down(start_all(to_down[1:]))

    def put(x_ref, t, value):
        x_ref[t, :, C : 2 * C] = value.astype(BF16)
        x_ref[t, :, 0:C] = pltpu.roll(value, 1, 0).astype(BF16)
        x_ref[t, :, 2 * C :] = pltpu.roll(value, TW - 1, 0).astype(BF16)

    step = 6
    for i in range(0, TH, step):
        part = jnp.dot(
            lhs[slot][i : i + step, :, tail].reshape(step * TW, PASS), rhs,
            preferred_element_type=F32,
        ).reshape(step, TW, C)
        for k in range(step):
            put(grid_x, i + k + 2, scaled(acc[i + k] + part[k], i + k + 2))

    def conv(x_ref, weight, starts):
        window = jnp.concatenate(
            [
                jnp.concatenate([x_ref[s + a] for s in starts], axis=0)
                for a in range(3)
            ],
            axis=1,
        )
        return jnp.dot(window, weight[...], preferred_element_type=F32).reshape(len(starts), TW, C)

    def silu(value):
        return value / (1.0 + jnp.exp(-value))

    def hide(lines):
        total = conv(grid_x, wone_v, lines)
        for k, s in enumerate(lines):
            put(hid_x, s, silu(total[k]))

    def hide_sides():
        shifted = []
        for c in range(8):
            value = sides[c]
            shifted.append(
                [(value if a == 0 else pltpu.roll(value, SIDE - a, 0)).astype(BF16) for a in range(3)]
            )
        window = jnp.concatenate(
            [
                jnp.concatenate([shifted[c + b][a] for a in range(3) for b in range(3)], axis=1)
                for c in (0, 1, 4, 5)
            ],
            axis=0,
        )
        total = silu(jnp.dot(window, wone_v[...], preferred_element_type=F32))
        ids = lax.broadcasted_iota(jnp.int32, (SIDE, C), 0)
        keep = ((ids > 0) | (lat > 0)) & ((ids < TH + 1) | (lat < lat_n - 1))
        for k in range(4):
            hid_side[k] = jnp.where(keep, total[SIDE * k : SIDE * (k + 1)], 0.0)

    ids16 = lax.broadcasted_iota(jnp.int32, (16, C), 0)

    def patch(s):
        before, first, final, after = (hid_side[k, s : s + 1] for k in range(4))

        def edit(lines, lanes, picks):
            value = hid_x[s, lines, lanes].astype(F32)
            for at, line in picks:
                value = jnp.where(ids16 == at, line, value)
            hid_x[s, lines, lanes] = value.astype(BF16)

        low, high = slice(0, 16), slice(TW - 16, TW)
        edit(low, slice(0, C), ((0, before), (1, first)))
        edit(low, slice(C, 2 * C), ((0, first),))
        edit(high, slice(C, 2 * C), ((15, final),))
        edit(high, slice(2 * C, 3 * C), ((14, final), (15, after)))

    def out_copy(lo, size):
        span = pl.ds(lo, size)
        return pltpu.make_async_copy(out_v.at[span], out.at[span], out_sem.at[lo])

    def encode(lines):
        total = conv(hid_x, wtwo_v, lines)
        for k, o in enumerate(lines):
            out_v[o] = (grid_x[o + 2, :, C : 2 * C].astype(F32) + total[k]).astype(BF16)

    weights[1].wait()
    for s in range(2, TH, 2):
        hide((s, s + 1))

    for item in beside:
        item.wait_recv()
    for k in range(2):
        sides[k] = col_in[0, k].astype(F32)
        sides[6 + k] = col_in[1, k].astype(F32)
    hide_sides()
    for s in range(2, TH):
        patch(s)
    weights[2].wait()
    for o in range(2, TH - 2, 2):
        encode((o, o + 1))
    out_copy(2, TH - 4).start()

    def outer(side):
        base = (0, TH + 2)[side]
        value = jnp.dot(
            mean_in[side].reshape(2 * TW, F), win_v[...], preferred_element_type=F32
        ).reshape(2, TW, C)
        turned = jnp.transpose(jnp.concatenate([log_in[side], jnp.zeros((120, 128), F32)], axis=0))
        for m in range(2):
            at = m if side == 0 else m + 2
            lg = jnp.broadcast_to(turned[:TW, at : at + 1], (TW, 128))
            line = value[m] + jnp.concatenate([lg, lg], axis=1) * w_dens[...]
            put(grid_x, base + m, line)
            for k, c in enumerate(COLS):
                sides[2 + k, base + m : base + m + 1] = line[c : c + 1]
        for k, c in enumerate((0, 1, 6, 7)):
            pair, line = k // 2, k % 2
            sides[c, base : base + 2] = corner_in[2 * side + pair, 2 * line : 2 * line + 2]

    def above():
        wait_all(log_down + to_down)()
        outer(0)

    def below():
        wait_all(log_up + to_up)()
        outer(1)

    when_up(above)
    when_down(below)

    @pl.when(lat == 0)
    def _():
        grid_x[0:2] = jnp.zeros((2, TW, 3 * C), BF16)

    @pl.when(lat == lat_n - 1)
    def _():
        grid_x[TH + 2 : TH + 4] = jnp.zeros((2, TW, 3 * C), BF16)

    hide((0, 1, TH, TH + 1))
    hide_sides()
    for s in (0, 1, TH, TH + 1):
        patch(s)

    @pl.when(lat == 0)
    def _():
        hid_x[0] = jnp.zeros((TW, 3 * C), BF16)

    @pl.when(lat == lat_n - 1)
    def _():
        hid_x[TH + 1] = jnp.zeros((TW, 3 * C), BF16)

    encode((0, 1, TH - 2, TH - 1))
    out_copy(0, 2).start()
    out_copy(TH - 2, 2).start()

    @pl.loop(1, n)
    def _(d):
        peer = across(d)
        cell_copy(d, peer).wait_send()
        row_copy(d, peer).wait_send()

    def drain(items):
        def act():
            for item in items:
                item.wait_send()
        return act

    drain(beside)()
    when_up(drain(log_up + to_up))
    when_down(drain(log_down + to_down))
    out_copy(2, TH - 4).wait()
    out_copy(0, 2).wait()
    out_copy(TH - 2, 2).wait()


def shards(features, cell_index, tile_rows, spread, w_in, w_dens, w_one, w_two):
    lat_n = lax.axis_size("lat")
    lon_n = lax.axis_size("lon")
    n = lat_n * lon_n
    hbm = pl.BlockSpec(memory_space=pltpu.HBM)
    anywhere = pl.BlockSpec(memory_space=pl.ANY)
    vmem = pl.BlockSpec(memory_space=pltpu.VMEM)
    smem = pl.BlockSpec(memory_space=pltpu.SMEM)
    dma = pltpu.SemaphoreType.DMA
    return pl.pallas_call(
        functools.partial(kernel, lat_n, lon_n),
        out_shape=jax.ShapeDtypeStruct((TH, TW, C), BF16),
        in_specs=[hbm, vmem, smem, smem, hbm, vmem, hbm, hbm],
        out_specs=anywhere,
        scratch_shapes=[
            pltpu.VMEM((n, 1, 128), jnp.int32),
            pltpu.VMEM((n, 1, 128), jnp.int32),
            pltpu.VMEM((n, CAP, F), BF16),
            pltpu.VMEM((3, TW, WIDE), BF16),
            pltpu.VMEM((PH, 16, WIDE), BF16),
            pltpu.VMEM((TH, TW, WIDE), BF16),
            pltpu.VMEM((TH, TW, WIDE), BF16),
            pltpu.VMEM((TH, TW, WIDE), BF16),
            pltpu.VMEM((SLOTS, 4 * SIDE, WIDE), BF16),
            pltpu.VMEM((TH, TW, C), F32),
            pltpu.VMEM((4 * SIDE, C), F32),
            pltpu.VMEM((4, TW, F), F32),
            pltpu.VMEM((SIDE, 128), F32),
            pltpu.VMEM((2, 8, 128), F32),
            pltpu.VMEM((2, 8, 128), F32),
            pltpu.VMEM((WIDE, C), BF16),
            pltpu.VMEM((TH, TW, 128), F32),
            pltpu.VMEM((TH, TW, 128), F32),
            pltpu.VMEM((TH + 4, TW, 3 * C), BF16),
            pltpu.VMEM((TH + 2, TW, 3 * C), BF16),
            pltpu.VMEM((2, 2, TW, F), BF16),
            pltpu.VMEM((2, 2, TW, F), BF16),
            pltpu.VMEM((4, SIDE, C), BF16),
            pltpu.VMEM((2, 2, SIDE, C), BF16),
            pltpu.VMEM((4, 8, C), F32),
            pltpu.VMEM((4, 8, C), F32),
            pltpu.VMEM((8, SIDE, C), F32),
            pltpu.VMEM((4, SIDE, C), F32),
            pltpu.VMEM((TH, TW, C), BF16),
            pltpu.VMEM((F, C), BF16),
            pltpu.VMEM((9 * C, C), BF16),
            pltpu.VMEM((9 * C, C), BF16),
            dma((n,)), dma((n,)), dma((n,)), dma((n,)),
            dma((2,)), dma((3,)), dma((TH,)), dma((10,)), dma((10,)),
        ],
        compiler_params=pltpu.CompilerParams(
            collective_id=0, has_side_effects=True, vmem_limit_bytes=60 * 1024 * 1024
        ),
    )(
        features.reshape(n, CAP, F), cell_index.reshape(-1, 128), tile_rows, spread, w_in, w_dens.reshape(1, C),
        w_one.reshape(9 * C, C), w_two.reshape(9 * C, C),
    )


def solution(mesh):
    blocks = P(("lat", "lon"))
    in_specs = (P(("lat", "lon"), None), blocks, blocks, P(), P(), P(), P(), P())
    out_specs = P("lat", "lon", None)
    return jax.shard_map(shards, mesh=mesh, in_specs=in_specs, out_specs=out_specs, check_vma=False)
```

```python
import functools

import jax
import jax.numpy as jnp
from jax import lax
from jax.experimental import pallas as pl
from jax.experimental.pallas import tpu as pltpu
from jax.sharding import PartitionSpec as P

TH = 24
TW = 96
F = 128
C = 256
CAP = 96
PH = 26
PW = 98
GROUP = 8
WIDE = GROUP * CAP
PASS = 256
BLOCKS = WIDE // 128
SLOTS = 4
VMEM = 67043328
HELD = 2 * C * (TH * TW + (TH + 4) * TW + 3 * (TH + 2) * TW + 9 * C)
SIDE = 32
COLS = (0, 1, TW - 2, TW - 1)
MESH = pl.DeviceIdType.MESH
F32 = jnp.float32
BF16 = jnp.bfloat16


def conv(x_ref, weight, starts):
    window = jnp.concatenate(
        [
            jnp.concatenate([x_ref[s + a] for s in starts], axis=0)
            for a in range(3)
        ],
        axis=1,
    )
    return jnp.dot(window, weight[...], preferred_element_type=F32).reshape(len(starts), TW, C)


def kernel(
    lat_n, lon_n,
    feats, raw, used, spread, w_in, w_dens, w_one, w_two, out_v, grid_x, hid_x, wtwo_v,
    cells, cells_in, rows_in, taps, hots, lhs0, lhs1, lhs2, lhs3, lhs_col, acc, acc_col, acc_row, count, log_in, log_out,
    rhs_v, inv_b, log_b, mean_out, mean_in, col_out, col_in, corner_out, corner_in, sides, hid_side,
    win_v, wone_v,
    row_send, row_recv, cell_send, cell_recv, own_sem, w_sem, halo_send, halo_recv,
):
    lhs = (lhs0, lhs1, lhs2, lhs3)
    n = lat_n * lon_n
    groups = n // GROUP
    lat = lax.axis_index("lat")
    lon = lax.axis_index("lon")
    me = lat * lon_n + lon
    east = (lon + 1) % lon_n
    west = (lon + lon_n - 1) % lon_n

    log_in[...] = jnp.zeros_like(log_in)
    bits = [1 << k for k in range(n.bit_length() - 1)]
    flips = [bit * (1 - 2 * (me // bit % 2)) for bit in bits]

    def across(d):
        return me + sum((d // bit % 2) * flip for bit, flip in zip(bits, flips))

    barrier = pltpu.get_barrier_semaphore()

    @pl.loop(1, n)
    def _(k):
        peer = (me + k) % n
        pl.semaphore_signal(
            barrier, inc=1, device_id=(peer // lon_n, peer % lon_n), device_id_type=MESH
        )

    weights = [
        pltpu.make_async_copy(w_in, win_v, w_sem.at[0]),
        pltpu.make_async_copy(w_one, wone_v, w_sem.at[1]),
        pltpu.make_async_copy(w_two, wtwo_v, w_sem.at[2]),
    ]
    for item in weights:
        item.start()

    lane = lax.broadcasted_iota(jnp.int32, (1, 128), 1)

    @pl.loop(0, n // 4)
    def _(quad):
        one, two, three = (raw[pl.ds(3 * quad + k, 1)] for k in range(3))
        picks = [
            one,
            jnp.where(lane < 32, pltpu.roll(one, 32, 1), pltpu.roll(two, 32, 1)),
            jnp.where(lane < 64, pltpu.roll(two, 64, 1), pltpu.roll(three, 64, 1)),
            pltpu.roll(three, 96, 1),
        ]
        for k, pick in enumerate(picks):
            row = ((pick.astype(F32) + 0.5) * (1.0 / PW)).astype(jnp.int32)
            code = row * 128 + (pick - row * PW)
            cells[4 * quad + k] = jnp.where(lane < used[4 * quad + k], code, 127 * 128)

    own = [
        pltpu.make_async_copy(feats.at[me], rows_in.at[0], own_sem.at[0]),
        pltpu.make_async_copy(cells.at[me], cells_in.at[0], own_sem.at[1]),
    ]
    count[...] = jnp.zeros_like(count)
    pl.semaphore_wait(barrier, n - 1)

    def cell_copy(d, peer):
        return pltpu.make_async_remote_copy(
            src_ref=cells.at[peer], dst_ref=cells_in.at[d],
            send_sem=cell_send.at[d], recv_sem=cell_recv.at[d],
            device_id=(peer // lon_n, peer % lon_n), device_id_type=MESH,
        )

    def row_copy(d, peer):
        return pltpu.make_async_remote_copy(
            src_ref=feats.at[peer], dst_ref=rows_in.at[d],
            send_sem=row_send.at[d], recv_sem=row_recv.at[d],
            device_id=(peer // lon_n, peer % lon_n), device_id_type=MESH,
        )

    for d in range(1, n):
        cell_copy(d, across(d)).start()
    for d in range(1, n):
        row_copy(d, across(d)).start()

    for item in own:
        item.start()

    def codes(group):
        enc = jnp.concatenate([cells_in[group * GROUP + m][:, :CAP] for m in range(GROUP)], axis=1)
        return enc & 127, enc >> 7

    def prepare(group, slot):
        col, row = codes(group)
        reach = jnp.broadcast_to(col, (TW, WIDE)) - lax.broadcasted_iota(jnp.int32, (TW, WIDE), 0)
        for a in range(3):
            tap = jnp.where(reach == 2, spread[a, 2], 0.0)
            tap = jnp.where(reach == 1, spread[a, 1], tap)
            taps[a] = jnp.where(reach == 0, spread[a, 0], tap).astype(BF16)
        wide_row = jnp.broadcast_to(row, (16, WIDE))
        for r in range(PH):
            hots[r] = jnp.where(wide_row == r, 1.0, 0.0).astype(BF16)
        above = jnp.broadcast_to(row, (SIDE, WIDE)) - lax.broadcasted_iota(jnp.int32, (SIDE, WIDE), 0)
        for k, c in enumerate(COLS):
            total = jnp.zeros((SIDE, WIDE), F32)
            for a in range(3):
                line = jnp.where(col == c + 2, spread[a, 2], 0.0)
                line = jnp.where(col == c + 1, spread[a, 1], line)
                line = jnp.where(col == c, spread[a, 0], line)
                total = jnp.where(above == a - 2, jnp.broadcast_to(line, (SIDE, WIDE)), total)
            lhs_col[slot, SIDE * k : SIDE * (k + 1)] = total.astype(BF16)

    def fill(block, slot):
        lanes = pl.ds(pl.multiple_of(block * 128, 128), 128)
        hot = [hots[r, :, lanes] for r in range(PH)]
        for strip in range(TW // 16):
            lines = slice(strip * 16, strip * 16 + 16)
            zero, one, two = (taps[a, lines, lanes] for a in range(3))
            for i in range(TH):
                lhs[slot][i, lines, lanes] = zero * hot[i] + one * hot[i + 1] + two * hot[i + 2]

    def build(group, slot):
        prepare(group, slot)

        @pl.loop(0, BLOCKS)
        def _(block):
            fill(block, slot)

    def cells_arrive(lo, hi):
        @pl.loop(lo, hi)
        def _(d):
            cell_copy(d, across(d)).wait_recv()

    own[1].wait()
    cells_arrive(1, GROUP)
    build(0, 0)
    if groups > 1:
        cells_arrive(GROUP, 2 * GROUP)
        build(1, 1)
    if groups > 2:
        cells_arrive(2 * GROUP, n)

    @pl.loop(0, groups)
    def _(group):
        col, row = codes(group)
        row_hot = jnp.where(
            lax.broadcasted_iota(jnp.int32, (SIDE, WIDE), 0) == row, 1.0, 0.0
        ).astype(BF16)
        col_hot = jnp.where(
            lax.broadcasted_iota(jnp.int32, (128, WIDE), 0) == col, 1.0, 0.0
        ).astype(BF16)
        count[...] += lax.dot_general(
            row_hot, col_hot, (((1,), (1,)), ((), ())), preferred_element_type=F32
        )

    density = jnp.zeros((SIDE, 128), F32)
    for a in range(3):
        line = count[...] if a == 2 else pltpu.roll(count[...], 2 - a, 0)
        for b in range(3):
            density += spread[a, b] * (line if b == 0 else pltpu.roll(line, 128 - b, 1))
    level = 1.0 + density
    inverse = 1.0 / level
    logs = jnp.log(level)
    log_out[0] = logs[0:8]
    log_out[1] = logs[SIDE - 8 : SIDE]

    def halo_copy(kind, src, dst, where):
        return pltpu.make_async_remote_copy(
            src_ref=src, dst_ref=dst, send_sem=halo_send.at[kind], recv_sem=halo_recv.at[kind],
            device_id=where, device_id_type=MESH,
        )

    up, down = lat - 1, lat + 1
    log_up = [halo_copy(0, log_out.at[0], log_in.at[1], (up, lon))]
    log_down = [halo_copy(1, log_out.at[1], log_in.at[0], (down, lon))]
    to_up = [
        halo_copy(2, mean_out.at[0], mean_in.at[1], (up, lon)),
        halo_copy(6, corner_out.at[0], corner_in.at[2], (up, east)),
        halo_copy(7, corner_out.at[1], corner_in.at[3], (up, west)),
    ]
    to_down = [
        halo_copy(3, mean_out.at[1], mean_in.at[0], (down, lon)),
        halo_copy(8, corner_out.at[2], corner_in.at[0], (down, east)),
        halo_copy(9, corner_out.at[3], corner_in.at[1], (down, west)),
    ]
    beside = [
        halo_copy(4, col_out.at[pl.ds(2, 2)], col_in.at[0], (lat, east)),
        halo_copy(5, col_out.at[pl.ds(0, 2)], col_in.at[1], (lat, west)),
    ]

    def when_up(act):
        @pl.when(lat > 0)
        def _():
            act()

    def when_down(act):
        @pl.when(lat < lat_n - 1)
        def _():
            act()

    def start_all(items):
        def act():
            for item in items:
                item.start()
        return act

    when_up(start_all(log_up))
    when_down(start_all(log_down))

    def features_of(group, lo, size):
        low, high = lo // CAP, -(-(lo + size) // CAP)
        rows = rows_in[pl.ds(group * GROUP + low, high - low)].reshape((high - low) * CAP, F)
        return rows[lo - low * CAP : lo - low * CAP + size]

    def add(group, slot, lo, size, first):
        rows = features_of(group, lo, size)
        span = slice(lo, lo + size)
        rhs = jnp.dot(rows, win_v[...], preferred_element_type=F32).astype(BF16)
        step = 12
        for i in range(0, TH, step):
            part = jnp.dot(
                lhs[slot][i : i + step, :, span].reshape(step * TW, size), rhs,
                preferred_element_type=F32,
            ).reshape(step, TW, C)
            acc[i : i + step] = part if first else acc[i : i + step] + part
        add_border(slot, rows, rhs, span, first)

    def add_beside(group, slot, later, spare, first):
        rows = features_of(group, 0, WIDE)
        rhs_v[...] = jnp.dot(rows, win_v[...], preferred_element_type=F32).astype(BF16)
        prepare(later, spare)
        size = TH // BLOCKS

        @pl.loop(0, BLOCKS)
        def _(block):
            lines = pl.ds(block * size, size)
            part = jnp.dot(
                lhs[slot][lines].reshape(size * TW, WIDE), rhs_v[...], preferred_element_type=F32
            ).reshape(size, TW, C)
            acc[lines] = part if first else acc[lines] + part
            fill(block, spare)

        add_border(slot, rows, rhs_v[...], slice(0, WIDE), first)

    def add_border(slot, rows, rhs, span, first):
        part = jnp.dot(lhs_col[slot, :, span], rhs, preferred_element_type=F32)
        acc_col[...] = part if first else acc_col[...] + part
        size = rows.shape[0]
        for k, i in ((0, 0), (2, TH - 2)):
            part = jnp.dot(
                lhs[slot][i : i + 2, :, span].reshape(2 * TW, size), rows,
                preferred_element_type=F32,
            ).reshape(2, TW, F)
            acc_row[k : k + 2] = part if first else acc_row[k : k + 2] + part

    def arrive(d):
        row_copy(d, across(d)).wait_recv()

    weights[0].wait()

    def wait_all(items):
        def act():
            for item in items:
                item.wait_recv()
        return act

    own[0].wait()
    if groups > 2:
        for d in range(1, GROUP):
            arrive(d)
        add_beside(0, 0, 2, 2, True)

    turned = jnp.transpose(jnp.concatenate([logs, jnp.zeros((128 - SIDE, 128), F32)], axis=0))
    for i in range(TH):
        log_b[i] = jnp.broadcast_to(turned[:TW, i + 2 : i + 3], (TW, 128))
    turned = jnp.transpose(
        jnp.concatenate([inverse, jnp.zeros((128 - SIDE, 128), F32)], axis=0)
    )
    for i in range(TH):
        inv_b[i] = jnp.broadcast_to(turned[:TW, i + 2 : i + 3], (TW, 128))

    if groups > 3:
        build(3, 3)
    for group in range(1, groups - 2):
        for m in range(GROUP):
            arrive(group * GROUP + m)
        later = group + 3
        if later < groups:
            add_beside(group, group % SLOTS, later, later % SLOTS, False)
        else:
            add(group, group % SLOTS, 0, WIDE, False)

    last = groups - 1
    slot = last % SLOTS
    for group in range(max(groups - 2, 0), groups):
        ready = 1 if group == 0 else 0
        for lo in range(0, WIDE - (PASS if group == last else 0), PASS):
            need = -(-(lo + PASS) // CAP)
            for m in range(ready, need):
                arrive(group * GROUP + m)
            ready = need
            add(group, group % SLOTS, lo, PASS, group == 0 and lo == 0)
    for m in range(ready, GROUP):
        arrive(last * GROUP + m)
    tail = slice(WIDE - PASS, WIDE)
    rows = features_of(last, WIDE - PASS, PASS)
    rhs = jnp.dot(rows, win_v[...], preferred_element_type=F32).astype(BF16)

    def scaled(total, t):
        factor, lg = inv_b[t - 2], log_b[t - 2]
        return total * jnp.concatenate([factor, factor], axis=1) + jnp.concatenate(
            [lg, lg], axis=1
        ) * w_dens[...]

    for k, i in ((0, 0), (2, TH - 2)):
        part = jnp.dot(
            lhs[slot][i : i + 2, :, tail].reshape(2 * TW, PASS), rows, preferred_element_type=F32
        ).reshape(2, TW, F)
        for m in range(2):
            mean_out[k // 2, m] = ((acc_row[k + m] + part[m]) * inv_b[i + m]).astype(BF16)
    when_up(to_up[0].start)
    when_down(to_down[0].start)
    part = acc_col[...] + jnp.dot(lhs_col[slot, :, tail], rhs, preferred_element_type=F32)
    inside = lax.broadcasted_iota(jnp.int32, (SIDE, C), 0)
    inside = (inside >= 2) & (inside < TH + 2)
    border = []
    for k, c in enumerate(COLS):
        factor = jnp.broadcast_to(inverse[:, c : c + 1], (SIDE, C))
        lg = jnp.broadcast_to(logs[:, c : c + 1], (SIDE, C))
        value = part[SIDE * k : SIDE * (k + 1)] * factor + lg * w_dens[...]
        value = jnp.where(inside, value, 0.0)
        border.append(value)
        col_out[k] = value.astype(BF16)
        sides[2 + k] = value
    for item in beside:
        item.start()
    pad = jnp.zeros((4, C), F32)
    for k, (line, pair) in enumerate(((2, 2), (2, 0), (TH, 2), (TH, 0))):
        corner_out[k] = jnp.concatenate(
            [border[pair][line : line + 2], border[pair + 1][line : line + 2], pad], axis=0
        )
    when_up(start_all(to_up[1:]))
    when_down(start_all(to_down[1:]))

    def put(x_ref, t, value):
        x_ref[t, :, C : 2 * C] = value.astype(BF16)
        x_ref[t, :, 0:C] = pltpu.roll(value, 1, 0).astype(BF16)
        x_ref[t, :, 2 * C :] = pltpu.roll(value, TW - 1, 0).astype(BF16)

    step = 6
    for i in range(0, TH, step):
        part = jnp.dot(
            lhs[slot][i : i + step, :, tail].reshape(step * TW, PASS), rhs,
            preferred_element_type=F32,
        ).reshape(step, TW, C)
        for k in range(step):
            grid_x[i + k + 2] = scaled(acc[i + k] + part[k], i + k + 2).astype(BF16)

    def silu(value):
        return value / (1.0 + jnp.exp(-value))

    def hide(lines):
        window = jnp.concatenate(
            [jnp.concatenate([grid_x[s + a] for s in lines], axis=0) for a in range(3)], axis=1
        )
        left, middle, right = (
            jnp.dot(
                window,
                jnp.concatenate([wone_v[(3 * a + b) * C : (3 * a + b + 1) * C] for a in range(3)], axis=0),
                preferred_element_type=F32,
            ).reshape(len(lines), TW, C)
            for b in range(3)
        )
        for k, s in enumerate(lines):
            total = pltpu.roll(left[k], 1, 0) + middle[k] + pltpu.roll(right[k], TW - 1, 0)
            put(hid_x, s, silu(total))

    def hide_sides():
        shifted = []
        for c in range(8):
            value = sides[c]
            shifted.append(
                [(value if a == 0 else pltpu.roll(value, SIDE - a, 0)).astype(BF16) for a in range(3)]
            )
        window = jnp.concatenate(
            [
                jnp.concatenate([shifted[c + b][a] for a in range(3) for b in range(3)], axis=1)
                for c in (0, 1, 4, 5)
            ],
            axis=0,
        )
        total = silu(jnp.dot(window, wone_v[...], preferred_element_type=F32))
        ids = lax.broadcasted_iota(jnp.int32, (SIDE, C), 0)
        keep = ((ids > 0) | (lat > 0)) & ((ids < TH + 1) | (lat < lat_n - 1))
        for k in range(4):
            hid_side[k] = jnp.where(keep, total[SIDE * k : SIDE * (k + 1)], 0.0)

    ids16 = lax.broadcasted_iota(jnp.int32, (16, C), 0)

    def patch(s):
        before, first, final, after = (hid_side[k, s : s + 1] for k in range(4))

        def edit(lines, lanes, picks):
            value = hid_x[s, lines, lanes].astype(F32)
            for at, line in picks:
                value = jnp.where(ids16 == at, line, value)
            hid_x[s, lines, lanes] = value.astype(BF16)

        low, high = slice(0, 16), slice(TW - 16, TW)
        edit(low, slice(0, C), ((0, before), (1, first)))
        edit(low, slice(C, 2 * C), ((0, first),))
        edit(high, slice(C, 2 * C), ((15, final),))
        edit(high, slice(2 * C, 3 * C), ((14, final), (15, after)))

    def encode(lines):
        total = conv(hid_x, wtwo_v, lines)
        for k, o in enumerate(lines):
            out_v[o] = (grid_x[o + 2].astype(F32) + total[k]).astype(BF16)

    weights[1].wait()
    for s in range(2, TH, 2):
        hide((s, s + 1))

    for item in beside:
        item.wait_recv()
    for k in range(2):
        sides[k] = col_in[0, k].astype(F32)
        sides[6 + k] = col_in[1, k].astype(F32)
    hide_sides()
    for s in range(2, TH):
        patch(s)
    weights[2].wait()
    for o in range(2, TH - 2, 2):
        encode((o, o + 1))

    def outer(side):
        base = (0, TH + 2)[side]
        value = jnp.dot(
            mean_in[side].reshape(2 * TW, F), win_v[...], preferred_element_type=F32
        ).reshape(2, TW, C)
        turned = jnp.transpose(jnp.concatenate([log_in[side], jnp.zeros((120, 128), F32)], axis=0))
        for m in range(2):
            at = m if side == 0 else m + 2
            lg = jnp.broadcast_to(turned[:TW, at : at + 1], (TW, 128))
            line = value[m] + jnp.concatenate([lg, lg], axis=1) * w_dens[...]
            grid_x[base + m] = line.astype(BF16)
            for k, c in enumerate(COLS):
                sides[2 + k, base + m : base + m + 1] = line[c : c + 1]
        for k, c in enumerate((0, 1, 6, 7)):
            pair, line = k // 2, k % 2
            sides[c, base : base + 2] = corner_in[2 * side + pair, 2 * line : 2 * line + 2]

    def above():
        wait_all(log_down + to_down)()
        outer(0)

    def below():
        wait_all(log_up + to_up)()
        outer(1)

    when_up(above)
    when_down(below)

    @pl.when(lat == 0)
    def _():
        grid_x[0:2] = jnp.zeros((2, TW, C), BF16)

    @pl.when(lat == lat_n - 1)
    def _():
        grid_x[TH + 2 : TH + 4] = jnp.zeros((2, TW, C), BF16)

    hide((0, 1, TH, TH + 1))
    hide_sides()
    for s in (0, 1, TH, TH + 1):
        patch(s)

    @pl.when(lat == 0)
    def _():
        hid_x[0] = jnp.zeros((TW, 3 * C), BF16)

    @pl.when(lat == lat_n - 1)
    def _():
        hid_x[TH + 1] = jnp.zeros((TW, 3 * C), BF16)

    @pl.loop(1, n)
    def _(d):
        peer = across(d)
        cell_copy(d, peer).wait_send()
        row_copy(d, peer).wait_send()

    def drain(items):
        def act():
            for item in items:
                item.wait_send()
        return act

    drain(beside)()
    when_up(drain(log_up + to_up))
    when_down(drain(log_down + to_down))


def finish(inner, grid_x, hid_x, weight, out, outer, sem):
    def copy(src, lo, size, k):
        return pltpu.make_async_copy(src, out.at[pl.ds(lo, size)], sem.at[k])

    copies = [
        copy(inner.at[pl.ds(2, TH - 4)], 2, TH - 4, 0),
        copy(outer.at[pl.ds(0, 2)], 0, 2, 1),
        copy(outer.at[pl.ds(2, 2)], TH - 2, 2, 2),
    ]
    copies[0].start()
    lines = (0, 1, TH - 2, TH - 1)
    total = conv(hid_x, weight, lines)
    for k, o in enumerate(lines):
        outer[k] = (grid_x[o + 2].astype(F32) + total[k]).astype(BF16)
    for item in copies[1:]:
        item.start()
    for item in copies:
        item.wait()


def shards(features, cell_index, tile_rows, spread, w_in, w_dens, w_one, w_two):
    lat_n = lax.axis_size("lat")
    lon_n = lax.axis_size("lon")
    n = lat_n * lon_n
    hbm = pl.BlockSpec(memory_space=pltpu.HBM)
    anywhere = pl.BlockSpec(memory_space=pl.ANY)
    vmem = pl.BlockSpec(memory_space=pltpu.VMEM)
    smem = pl.BlockSpec(memory_space=pltpu.SMEM)
    dma = pltpu.SemaphoreType.DMA
    held = pl.pallas_call(
        functools.partial(kernel, lat_n, lon_n),
        out_shape=[
            pltpu.VMEM((TH, TW, C), BF16),
            pltpu.VMEM((TH + 4, TW, C), BF16),
            pltpu.VMEM((TH + 2, TW, 3 * C), BF16),
            pltpu.VMEM((9 * C, C), BF16),
        ],
        in_specs=[hbm, vmem, smem, smem, hbm, vmem, hbm, hbm],
        out_specs=[vmem] * 4,
        scratch_shapes=[
            pltpu.VMEM((n, 1, 128), jnp.int32),
            pltpu.VMEM((n, 1, 128), jnp.int32),
            pltpu.VMEM((n, CAP, F), BF16),
            pltpu.VMEM((3, TW, WIDE), BF16),
            pltpu.VMEM((PH, 16, WIDE), BF16),
            pltpu.VMEM((TH, TW, WIDE), BF16),
            pltpu.VMEM((TH, TW, WIDE), BF16),
            pltpu.VMEM((TH, TW, WIDE), BF16),
            pltpu.VMEM((TH, TW, WIDE), BF16),
            pltpu.VMEM((SLOTS, 4 * SIDE, WIDE), BF16),
            pltpu.VMEM((TH, TW, C), F32),
            pltpu.VMEM((4 * SIDE, C), F32),
            pltpu.VMEM((4, TW, F), F32),
            pltpu.VMEM((SIDE, 128), F32),
            pltpu.VMEM((2, 8, 128), F32),
            pltpu.VMEM((2, 8, 128), F32),
            pltpu.VMEM((WIDE, C), BF16),
            pltpu.VMEM((TH, TW, 128), F32),
            pltpu.VMEM((TH, TW, 128), F32),
            pltpu.VMEM((2, 2, TW, F), BF16),
            pltpu.VMEM((2, 2, TW, F), BF16),
            pltpu.VMEM((4, SIDE, C), BF16),
            pltpu.VMEM((2, 2, SIDE, C), BF16),
            pltpu.VMEM((4, 8, C), F32),
            pltpu.VMEM((4, 8, C), F32),
            pltpu.VMEM((8, SIDE, C), F32),
            pltpu.VMEM((4, SIDE, C), F32),
            pltpu.VMEM((F, C), BF16),
            pltpu.VMEM((9 * C, C), BF16),
            dma((n,)), dma((n,)), dma((n,)), dma((n,)),
            dma((2,)), dma((3,)), dma((10,)), dma((10,)),
        ],
        compiler_params=pltpu.CompilerParams(
            collective_id=0, has_side_effects=True, vmem_limit_bytes=VMEM - HELD
        ),
    )(
        features.reshape(n, CAP, F), cell_index.reshape(-1, 128), tile_rows, spread, w_in, w_dens.reshape(1, C),
        w_one.reshape(9 * C, C), w_two.reshape(9 * C, C),
    )
    return pl.pallas_call(
        finish,
        out_shape=jax.ShapeDtypeStruct((TH, TW, C), BF16),
        in_specs=[vmem] * 4,
        out_specs=anywhere,
        scratch_shapes=[pltpu.VMEM((4, TW, C), BF16), dma((3,))],
        compiler_params=pltpu.CompilerParams(vmem_limit_bytes=16 * 1024 * 1024),
    )(*held)


def solution(mesh):
    blocks = P(("lat", "lon"))
    in_specs = (P(("lat", "lon"), None), blocks, blocks, P(), P(), P(), P(), P())
    out_specs = P("lat", "lon", None)
    return jax.shard_map(shards, mesh=mesh, in_specs=in_specs, out_specs=out_specs, check_vma=False)
```

```python
import functools

import jax
import jax.numpy as jnp
from jax import lax
from jax.experimental import pallas as pl
from jax.experimental.pallas import tpu as pltpu
from jax.sharding import PartitionSpec as P

TH = 24
TW = 96
F = 128
C = 256
CAP = 96
PH = 26
PW = 98
GROUP = 8
WIDE = GROUP * CAP
PASS = WIDE // 2
BLOCKS = WIDE // 128
SLOTS = 4
VMEM = 67043328
HELD = 2 * C * (TH * TW + (TH + 4) * TW + 3 * (TH + 2) * TW + 9 * C)
SIDE = 32
COLS = (0, 1, TW - 2, TW - 1)
MESH = pl.DeviceIdType.MESH
F32 = jnp.float32
BF16 = jnp.bfloat16


def conv(x_ref, weight, starts):
    window = jnp.concatenate(
        [
            jnp.concatenate([x_ref[s + a] for s in starts], axis=0)
            for a in range(3)
        ],
        axis=1,
    )
    return jnp.dot(window, weight[...], preferred_element_type=F32).reshape(len(starts), TW, C)


def kernel(
    lat_n, lon_n,
    feats, raw, used, spread, w_in, w_dens, w_one, w_two, out_v, grid_x, hid_x, wtwo_v,
    cells, cells_in, rows_in, taps, hots, lhs0, lhs1, lhs2, lhs3, lhs_col, acc, acc_col, acc_row, count, log_in, log_out,
    rhs_v, inv_b, log_b, mean_out, mean_in, col_out, col_in, corner_out, corner_in, sides, hid_side,
    win_v, wone_v,
    row_send, row_recv, cell_send, cell_recv, own_sem, w_sem, halo_send, halo_recv,
):
    lhs = (lhs0, lhs1, lhs2, lhs3)
    n = lat_n * lon_n
    groups = n // GROUP
    lat = lax.axis_index("lat")
    lon = lax.axis_index("lon")
    me = lat * lon_n + lon
    east = (lon + 1) % lon_n
    west = (lon + lon_n - 1) % lon_n

    log_in[...] = jnp.zeros_like(log_in)
    bits = [1 << k for k in range(n.bit_length() - 1)]
    flips = [bit * (1 - 2 * (me // bit % 2)) for bit in bits]

    def across(d):
        return me + sum((d // bit % 2) * flip for bit, flip in zip(bits, flips))

    barrier = pltpu.get_barrier_semaphore()

    @pl.loop(1, n)
    def _(k):
        peer = (me + k) % n
        pl.semaphore_signal(
            barrier, inc=1, device_id=(peer // lon_n, peer % lon_n), device_id_type=MESH
        )

    weights = [
        pltpu.make_async_copy(w_in, win_v, w_sem.at[0]),
        pltpu.make_async_copy(w_one, wone_v, w_sem.at[1]),
        pltpu.make_async_copy(w_two, wtwo_v, w_sem.at[2]),
    ]
    for item in weights:
        item.start()

    lane = lax.broadcasted_iota(jnp.int32, (1, 128), 1)

    @pl.loop(0, n // 4)
    def _(quad):
        one, two, three = (raw[pl.ds(3 * quad + k, 1)] for k in range(3))
        picks = [
            one,
            jnp.where(lane < 32, pltpu.roll(one, 32, 1), pltpu.roll(two, 32, 1)),
            jnp.where(lane < 64, pltpu.roll(two, 64, 1), pltpu.roll(three, 64, 1)),
            pltpu.roll(three, 96, 1),
        ]
        for k, pick in enumerate(picks):
            row = ((pick.astype(F32) + 0.5) * (1.0 / PW)).astype(jnp.int32)
            code = row * 128 + (pick - row * PW)
            cells[4 * quad + k] = jnp.where(lane < used[4 * quad + k], code, 127 * 128)

    own = [
        pltpu.make_async_copy(feats.at[me], rows_in.at[0], own_sem.at[0]),
        pltpu.make_async_copy(cells.at[me], cells_in.at[0], own_sem.at[1]),
    ]
    count[...] = jnp.zeros_like(count)
    pl.semaphore_wait(barrier, n - 1)

    def cell_copy(d, peer):
        return pltpu.make_async_remote_copy(
            src_ref=cells.at[peer], dst_ref=cells_in.at[d],
            send_sem=cell_send.at[d], recv_sem=cell_recv.at[d],
            device_id=(peer // lon_n, peer % lon_n), device_id_type=MESH,
        )

    def row_copy(d, peer):
        return pltpu.make_async_remote_copy(
            src_ref=feats.at[peer], dst_ref=rows_in.at[d],
            send_sem=row_send.at[d], recv_sem=row_recv.at[d],
            device_id=(peer // lon_n, peer % lon_n), device_id_type=MESH,
        )

    for d in range(1, n):
        cell_copy(d, across(d)).start()
    for d in range(1, n):
        row_copy(d, across(d)).start()

    for item in own:
        item.start()

    def codes(group):
        enc = jnp.concatenate([cells_in[group * GROUP + m][:, :CAP] for m in range(GROUP)], axis=1)
        return enc & 127, enc >> 7

    def prepare(group, slot):
        col, row = codes(group)
        reach = jnp.broadcast_to(col, (TW, WIDE)) - lax.broadcasted_iota(jnp.int32, (TW, WIDE), 0)
        for a in range(3):
            tap = jnp.where(reach == 2, spread[a, 2], 0.0)
            tap = jnp.where(reach == 1, spread[a, 1], tap)
            taps[a] = jnp.where(reach == 0, spread[a, 0], tap).astype(BF16)
        wide_row = jnp.broadcast_to(row, (16, WIDE))
        for r in range(PH):
            hots[r] = jnp.where(wide_row == r, 1.0, 0.0).astype(BF16)
        above = jnp.broadcast_to(row, (SIDE, WIDE)) - lax.broadcasted_iota(jnp.int32, (SIDE, WIDE), 0)
        for k, c in enumerate(COLS):
            total = jnp.zeros((SIDE, WIDE), F32)
            for a in range(3):
                line = jnp.where(col == c + 2, spread[a, 2], 0.0)
                line = jnp.where(col == c + 1, spread[a, 1], line)
                line = jnp.where(col == c, spread[a, 0], line)
                total = jnp.where(above == a - 2, jnp.broadcast_to(line, (SIDE, WIDE)), total)
            lhs_col[slot, SIDE * k : SIDE * (k + 1)] = total.astype(BF16)

    def fill(block, slot):
        lanes = pl.ds(pl.multiple_of(block * 128, 128), 128)
        hot = [hots[r, :, lanes] for r in range(PH)]
        for strip in range(TW // 16):
            lines = slice(strip * 16, strip * 16 + 16)
            zero, one, two = (taps[a, lines, lanes] for a in range(3))
            for i in range(TH):
                lhs[slot][i, lines, lanes] = zero * hot[i] + one * hot[i + 1] + two * hot[i + 2]

    def build(group, slot):
        prepare(group, slot)

        @pl.loop(0, BLOCKS)
        def _(block):
            fill(block, slot)

    def cells_arrive(lo, hi):
        for d in range(lo, hi):
            cell_copy(d, across(d)).wait_recv()

    own[1].wait()
    cells_arrive(1, GROUP)
    build(0, 0)
    if groups > 1:
        cells_arrive(GROUP, 2 * GROUP)
        build(1, 1)
    if groups > 2:
        cells_arrive(2 * GROUP, n)

    @pl.loop(0, groups)
    def _(group):
        col, row = codes(group)
        row_hot = jnp.where(
            lax.broadcasted_iota(jnp.int32, (SIDE, WIDE), 0) == row, 1.0, 0.0
        ).astype(BF16)
        col_hot = jnp.where(
            lax.broadcasted_iota(jnp.int32, (128, WIDE), 0) == col, 1.0, 0.0
        ).astype(BF16)
        count[...] += lax.dot_general(
            row_hot, col_hot, (((1,), (1,)), ((), ())), preferred_element_type=F32
        )

    density = jnp.zeros((SIDE, 128), F32)
    for a in range(3):
        line = count[...] if a == 2 else pltpu.roll(count[...], 2 - a, 0)
        for b in range(3):
            density += spread[a, b] * (line if b == 0 else pltpu.roll(line, 128 - b, 1))
    level = 1.0 + density
    inverse = 1.0 / level
    logs = jnp.log(level)
    log_out[0] = logs[0:8]
    log_out[1] = logs[SIDE - 8 : SIDE]

    def halo_copy(kind, src, dst, where):
        return pltpu.make_async_remote_copy(
            src_ref=src, dst_ref=dst, send_sem=halo_send.at[kind], recv_sem=halo_recv.at[kind],
            device_id=where, device_id_type=MESH,
        )

    up, down = lat - 1, lat + 1
    log_up = [halo_copy(0, log_out.at[0], log_in.at[1], (up, lon))]
    log_down = [halo_copy(1, log_out.at[1], log_in.at[0], (down, lon))]
    to_up = [
        halo_copy(2, mean_out.at[0], mean_in.at[1], (up, lon)),
        halo_copy(6, corner_out.at[0], corner_in.at[2], (up, east)),
        halo_copy(7, corner_out.at[1], corner_in.at[3], (up, west)),
    ]
    to_down = [
        halo_copy(3, mean_out.at[1], mean_in.at[0], (down, lon)),
        halo_copy(8, corner_out.at[2], corner_in.at[0], (down, east)),
        halo_copy(9, corner_out.at[3], corner_in.at[1], (down, west)),
    ]
    beside = [
        halo_copy(4, col_out.at[pl.ds(2, 2)], col_in.at[0], (lat, east)),
        halo_copy(5, col_out.at[pl.ds(0, 2)], col_in.at[1], (lat, west)),
    ]

    def when_up(act):
        @pl.when(lat > 0)
        def _():
            act()

    def when_down(act):
        @pl.when(lat < lat_n - 1)
        def _():
            act()

    def start_all(items):
        def act():
            for item in items:
                item.start()
        return act

    when_up(start_all(log_up))
    when_down(start_all(log_down))

    def features_of(group, lo, size):
        low, high = lo // CAP, -(-(lo + size) // CAP)
        rows = rows_in[pl.ds(group * GROUP + low, high - low)].reshape((high - low) * CAP, F)
        return rows[lo - low * CAP : lo - low * CAP + size]

    def add(group, slot, lo, size, first):
        rows = features_of(group, lo, size)
        span = slice(lo, lo + size)
        rhs = jnp.dot(rows, win_v[...], preferred_element_type=F32).astype(BF16)
        step = 12
        for i in range(0, TH, step):
            part = jnp.dot(
                lhs[slot][i : i + step, :, span].reshape(step * TW, size), rhs,
                preferred_element_type=F32,
            ).reshape(step, TW, C)
            acc[i : i + step] = part if first else acc[i : i + step] + part
        add_border(slot, rows, rhs, span, first)

    def add_beside(group, slot, later, spare, first):
        rows = features_of(group, 0, WIDE)
        rhs_v[...] = jnp.dot(rows, win_v[...], preferred_element_type=F32).astype(BF16)
        prepare(later, spare)
        size = TH // BLOCKS

        @pl.loop(0, BLOCKS)
        def _(block):
            lines = pl.ds(block * size, size)
            part = jnp.dot(
                lhs[slot][lines].reshape(size * TW, WIDE), rhs_v[...], preferred_element_type=F32
            ).reshape(size, TW, C)
            acc[lines] = part if first else acc[lines] + part
            fill(block, spare)

        add_border(slot, rows, rhs_v[...], slice(0, WIDE), first)

    def add_border(slot, rows, rhs, span, first):
        part = jnp.dot(lhs_col[slot, :, span], rhs, preferred_element_type=F32)
        acc_col[...] = part if first else acc_col[...] + part
        size = rows.shape[0]
        for k, i in ((0, 0), (2, TH - 2)):
            part = jnp.dot(
                lhs[slot][i : i + 2, :, span].reshape(2 * TW, size), rows,
                preferred_element_type=F32,
            ).reshape(2, TW, F)
            acc_row[k : k + 2] = part if first else acc_row[k : k + 2] + part

    def arrive(d):
        row_copy(d, across(d)).wait_recv()

    weights[0].wait()

    def wait_all(items):
        def act():
            for item in items:
                item.wait_recv()
        return act

    own[0].wait()
    if groups > 2:
        build(2, 2)
        for d in range(1, GROUP):
            arrive(d)
        if groups > 3:
            add_beside(0, 0, 3, 3, True)
        else:
            add(0, 0, 0, WIDE, True)

    turned = jnp.transpose(jnp.concatenate([logs, jnp.zeros((128 - SIDE, 128), F32)], axis=0))
    for i in range(TH):
        log_b[i] = jnp.broadcast_to(turned[:TW, i + 2 : i + 3], (TW, 128))
    turned = jnp.transpose(
        jnp.concatenate([inverse, jnp.zeros((128 - SIDE, 128), F32)], axis=0)
    )
    for i in range(TH):
        inv_b[i] = jnp.broadcast_to(turned[:TW, i + 2 : i + 3], (TW, 128))

    for group in range(1, groups - 2):
        for m in range(GROUP):
            arrive(group * GROUP + m)
        later = group + 3
        if later < groups:
            add_beside(group, group % SLOTS, later, later % SLOTS, False)
        else:
            add(group, group % SLOTS, 0, WIDE, False)

    last = groups - 1
    slot = last % SLOTS
    for group in range(max(groups - 2, 0), groups):
        ready = 1 if group == 0 else 0
        for lo in range(0, WIDE - (PASS if group == last else 0), PASS):
            need = -(-(lo + PASS) // CAP)
            for m in range(ready, need):
                arrive(group * GROUP + m)
            ready = need
            add(group, group % SLOTS, lo, PASS, group == 0 and lo == 0)
    for m in range(ready, GROUP):
        arrive(last * GROUP + m)
    tail = slice(WIDE - PASS, WIDE)
    rows = features_of(last, WIDE - PASS, PASS)
    rhs = jnp.dot(rows, win_v[...], preferred_element_type=F32).astype(BF16)

    def scaled(total, t):
        factor, lg = inv_b[t - 2], log_b[t - 2]
        return total * jnp.concatenate([factor, factor], axis=1) + jnp.concatenate(
            [lg, lg], axis=1
        ) * w_dens[...]

    for k, i in ((0, 0), (2, TH - 2)):
        part = jnp.dot(
            lhs[slot][i : i + 2, :, tail].reshape(2 * TW, PASS), rows, preferred_element_type=F32
        ).reshape(2, TW, F)
        for m in range(2):
            mean_out[k // 2, m] = ((acc_row[k + m] + part[m]) * inv_b[i + m]).astype(BF16)
    when_up(to_up[0].start)
    when_down(to_down[0].start)
    part = acc_col[...] + jnp.dot(lhs_col[slot, :, tail], rhs, preferred_element_type=F32)
    inside = lax.broadcasted_iota(jnp.int32, (SIDE, C), 0)
    inside = (inside >= 2) & (inside < TH + 2)
    border = []
    for k, c in enumerate(COLS):
        factor = jnp.broadcast_to(inverse[:, c : c + 1], (SIDE, C))
        lg = jnp.broadcast_to(logs[:, c : c + 1], (SIDE, C))
        value = part[SIDE * k : SIDE * (k + 1)] * factor + lg * w_dens[...]
        value = jnp.where(inside, value, 0.0)
        border.append(value)
        col_out[k] = value.astype(BF16)
        sides[2 + k] = value
    for item in beside:
        item.start()
    pad = jnp.zeros((4, C), F32)
    for k, (line, pair) in enumerate(((2, 2), (2, 0), (TH, 2), (TH, 0))):
        corner_out[k] = jnp.concatenate(
            [border[pair][line : line + 2], border[pair + 1][line : line + 2], pad], axis=0
        )
    when_up(start_all(to_up[1:]))
    when_down(start_all(to_down[1:]))

    def put(x_ref, t, value):
        x_ref[t, :, C : 2 * C] = value.astype(BF16)
        x_ref[t, :, 0:C] = pltpu.roll(value, 1, 0).astype(BF16)
        x_ref[t, :, 2 * C :] = pltpu.roll(value, TW - 1, 0).astype(BF16)

    step = 6
    for i in range(0, TH, step):
        part = jnp.dot(
            lhs[slot][i : i + step, :, tail].reshape(step * TW, PASS), rhs,
            preferred_element_type=F32,
        ).reshape(step, TW, C)
        for k in range(step):
            grid_x[i + k + 2] = scaled(acc[i + k] + part[k], i + k + 2).astype(BF16)

    def silu(value):
        return value / (1.0 + jnp.exp(-value))

    def hide(lines):
        window = jnp.concatenate(
            [jnp.concatenate([grid_x[s + a] for s in lines], axis=0) for a in range(3)], axis=1
        )
        left, middle, right = (
            jnp.dot(
                window,
                jnp.concatenate([wone_v[(3 * a + b) * C : (3 * a + b + 1) * C] for a in range(3)], axis=0),
                preferred_element_type=F32,
            ).reshape(len(lines), TW, C)
            for b in range(3)
        )
        for k, s in enumerate(lines):
            total = pltpu.roll(left[k], 1, 0) + middle[k] + pltpu.roll(right[k], TW - 1, 0)
            put(hid_x, s, silu(total))

    def hide_sides():
        shifted = []
        for c in range(8):
            value = sides[c]
            shifted.append(
                [(value if a == 0 else pltpu.roll(value, SIDE - a, 0)).astype(BF16) for a in range(3)]
            )
        window = jnp.concatenate(
            [
                jnp.concatenate([shifted[c + b][a] for a in range(3) for b in range(3)], axis=1)
                for c in (0, 1, 4, 5)
            ],
            axis=0,
        )
        total = silu(jnp.dot(window, wone_v[...], preferred_element_type=F32))
        ids = lax.broadcasted_iota(jnp.int32, (SIDE, C), 0)
        keep = ((ids > 0) | (lat > 0)) & ((ids < TH + 1) | (lat < lat_n - 1))
        for k in range(4):
            hid_side[k] = jnp.where(keep, total[SIDE * k : SIDE * (k + 1)], 0.0)

    ids16 = lax.broadcasted_iota(jnp.int32, (16, C), 0)

    def patch(s):
        before, first, final, after = (hid_side[k, s : s + 1] for k in range(4))

        def edit(lines, lanes, picks):
            value = hid_x[s, lines, lanes].astype(F32)
            for at, line in picks:
                value = jnp.where(ids16 == at, line, value)
            hid_x[s, lines, lanes] = value.astype(BF16)

        low, high = slice(0, 16), slice(TW - 16, TW)
        edit(low, slice(0, C), ((0, before), (1, first)))
        edit(low, slice(C, 2 * C), ((0, first),))
        edit(high, slice(C, 2 * C), ((15, final),))
        edit(high, slice(2 * C, 3 * C), ((14, final), (15, after)))

    def encode(lines):
        total = conv(hid_x, wtwo_v, lines)
        for k, o in enumerate(lines):
            out_v[o] = (grid_x[o + 2].astype(F32) + total[k]).astype(BF16)

    weights[1].wait()
    for s in range(2, TH, 2):
        hide((s, s + 1))

    for item in beside:
        item.wait_recv()
    for k in range(2):
        sides[k] = col_in[0, k].astype(F32)
        sides[6 + k] = col_in[1, k].astype(F32)
    hide_sides()
    for s in range(2, TH):
        patch(s)
    weights[2].wait()
    for o in range(2, TH - 2, 2):
        encode((o, o + 1))

    for d in range(1, n):
        cell_copy(d, across(d)).wait_send()
        row_copy(d, across(d)).wait_send()

    def outer(side):
        base = (0, TH + 2)[side]
        value = jnp.dot(
            mean_in[side].reshape(2 * TW, F), win_v[...], preferred_element_type=F32
        ).reshape(2, TW, C)
        turned = jnp.transpose(jnp.concatenate([log_in[side], jnp.zeros((120, 128), F32)], axis=0))
        for m in range(2):
            at = m if side == 0 else m + 2
            lg = jnp.broadcast_to(turned[:TW, at : at + 1], (TW, 128))
            line = value[m] + jnp.concatenate([lg, lg], axis=1) * w_dens[...]
            grid_x[base + m] = line.astype(BF16)
            for k, c in enumerate(COLS):
                sides[2 + k, base + m : base + m + 1] = line[c : c + 1]
        for k, c in enumerate((0, 1, 6, 7)):
            pair, line = k // 2, k % 2
            sides[c, base : base + 2] = corner_in[2 * side + pair, 2 * line : 2 * line + 2]

    def above():
        wait_all(log_down + to_down)()
        outer(0)

    def below():
        wait_all(log_up + to_up)()
        outer(1)

    when_up(above)
    when_down(below)

    @pl.when(lat == 0)
    def _():
        grid_x[0:2] = jnp.zeros((2, TW, C), BF16)

    @pl.when(lat == lat_n - 1)
    def _():
        grid_x[TH + 2 : TH + 4] = jnp.zeros((2, TW, C), BF16)

    hide((0, 1, TH, TH + 1))
    hide_sides()
    for s in (0, 1, TH, TH + 1):
        patch(s)

    @pl.when(lat == 0)
    def _():
        hid_x[0] = jnp.zeros((TW, 3 * C), BF16)

    @pl.when(lat == lat_n - 1)
    def _():
        hid_x[TH + 1] = jnp.zeros((TW, 3 * C), BF16)

    def drain(items):
        def act():
            for item in items:
                item.wait_send()
        return act

    drain(beside)()
    when_up(drain(log_up + to_up))
    when_down(drain(log_down + to_down))


def finish(inner, grid_x, hid_x, weight, out, outer, sem):
    def copy(src, lo, size, k):
        return pltpu.make_async_copy(src, out.at[pl.ds(lo, size)], sem.at[k])

    copies = [
        copy(inner.at[pl.ds(2, TH - 4)], 2, TH - 4, 0),
        copy(outer.at[pl.ds(0, 2)], 0, 2, 1),
        copy(outer.at[pl.ds(2, 2)], TH - 2, 2, 2),
    ]
    copies[0].start()
    lines = (0, 1, TH - 2, TH - 1)
    total = conv(hid_x, weight, lines)
    for k, o in enumerate(lines):
        outer[k] = (grid_x[o + 2].astype(F32) + total[k]).astype(BF16)
    for item in copies[1:]:
        item.start()
    for item in copies:
        item.wait()


def shards(features, cell_index, tile_rows, spread, w_in, w_dens, w_one, w_two):
    lat_n = lax.axis_size("lat")
    lon_n = lax.axis_size("lon")
    n = lat_n * lon_n
    hbm = pl.BlockSpec(memory_space=pltpu.HBM)
    anywhere = pl.BlockSpec(memory_space=pl.ANY)
    vmem = pl.BlockSpec(memory_space=pltpu.VMEM)
    smem = pl.BlockSpec(memory_space=pltpu.SMEM)
    dma = pltpu.SemaphoreType.DMA
    held = pl.pallas_call(
        functools.partial(kernel, lat_n, lon_n),
        out_shape=[
            pltpu.VMEM((TH, TW, C), BF16),
            pltpu.VMEM((TH + 4, TW, C), BF16),
            pltpu.VMEM((TH + 2, TW, 3 * C), BF16),
            pltpu.VMEM((9 * C, C), BF16),
        ],
        in_specs=[hbm, vmem, smem, smem, hbm, vmem, hbm, hbm],
        out_specs=[vmem] * 4,
        scratch_shapes=[
            pltpu.VMEM((n, 1, 128), jnp.int32),
            pltpu.VMEM((n, 1, 128), jnp.int32),
            pltpu.VMEM((n, CAP, F), BF16),
            pltpu.VMEM((3, TW, WIDE), BF16),
            pltpu.VMEM((PH, 16, WIDE), BF16),
            pltpu.VMEM((TH, TW, WIDE), BF16),
            pltpu.VMEM((TH, TW, WIDE), BF16),
            pltpu.VMEM((TH, TW, WIDE), BF16),
            pltpu.VMEM((TH, TW, WIDE), BF16),
            pltpu.VMEM((SLOTS, 4 * SIDE, WIDE), BF16),
            pltpu.VMEM((TH, TW, C), F32),
            pltpu.VMEM((4 * SIDE, C), F32),
            pltpu.VMEM((4, TW, F), F32),
            pltpu.VMEM((SIDE, 128), F32),
            pltpu.VMEM((2, 8, 128), F32),
            pltpu.VMEM((2, 8, 128), F32),
            pltpu.VMEM((WIDE, C), BF16),
            pltpu.VMEM((TH, TW, 128), F32),
            pltpu.VMEM((TH, TW, 128), F32),
            pltpu.VMEM((2, 2, TW, F), BF16),
            pltpu.VMEM((2, 2, TW, F), BF16),
            pltpu.VMEM((4, SIDE, C), BF16),
            pltpu.VMEM((2, 2, SIDE, C), BF16),
            pltpu.VMEM((4, 8, C), F32),
            pltpu.VMEM((4, 8, C), F32),
            pltpu.VMEM((8, SIDE, C), F32),
            pltpu.VMEM((4, SIDE, C), F32),
            pltpu.VMEM((F, C), BF16),
            pltpu.VMEM((9 * C, C), BF16),
            dma((n,)), dma((n,)), dma((n,)), dma((n,)),
            dma((2,)), dma((3,)), dma((10,)), dma((10,)),
        ],
        compiler_params=pltpu.CompilerParams(
            collective_id=0, has_side_effects=True, vmem_limit_bytes=VMEM - HELD
        ),
    )(
        features.reshape(n, CAP, F), cell_index.reshape(-1, 128), tile_rows, spread, w_in, w_dens.reshape(1, C),
        w_one.reshape(9 * C, C), w_two.reshape(9 * C, C),
    )
    return pl.pallas_call(
        finish,
        out_shape=jax.ShapeDtypeStruct((TH, TW, C), BF16),
        in_specs=[vmem] * 4,
        out_specs=anywhere,
        scratch_shapes=[pltpu.VMEM((4, TW, C), BF16), dma((3,))],
        compiler_params=pltpu.CompilerParams(vmem_limit_bytes=16 * 1024 * 1024),
    )(*held)


def solution(mesh):
    blocks = P(("lat", "lon"))
    in_specs = (P(("lat", "lon"), None), blocks, blocks, P(), P(), P(), P(), P())
    out_specs = P("lat", "lon", None)
    return jax.shard_map(shards, mesh=mesh, in_specs=in_specs, out_specs=out_specs, check_vma=False)
```
